32 devices in a mesh: expert: 32 (over z, y, x, core), latent: 1, mp: 1.
Axes of the slice: x: 2, y: 2, z: 4, core: 2. Of those that a mesh axis runs over, the one named last changes fastest.
Arguments:
- tokens: bfloat16 [8192, 2048], P('expert', 'mp'), may hold values from -6 to 6
- targets: bfloat16 [8192, 2048], P('expert', 'mp'), may hold values from -6 to 6
- expert_ids: int32 [8192, 1], P('expert'), may hold values from 0 to 31; in each aligned block of 256 rows (0 to 255, 256 to 511, ...) at most 16 rows name the same one
- latent_ids: int32 [8192, 32], P('expert'), may hold values from 0 to 8191, as said below
- w_enc: bfloat16 [32, 2048, 8192], P('expert', 'mp', 'latent'), may hold values from -0.125 to 0.125
- b_enc: float32 [32, 8192], P('expert', 'latent'), may hold values from -4 to 4
- w_dec: bfloat16 [32, 8192, 2048], P('expert', 'latent', 'mp'), may hold values from -1 to 1
- b_dec: float32 [32, 2048], P('expert', 'mp'), may hold values from -4 to 4
Outputs:
- rebuilt: bfloat16 [8192, 2048], P('expert', 'mp')
- grad_dec: bfloat16 [32, 8192, 2048], P('expert', 'latent', 'mp')
The draws below stay inside these ranges and needn't reach their ends.
Inputs may be any that keep to these rules, and one draw needn't show every extreme that they name: `expert_ids`: among the 256 rows of one index of expert no expert id occurs more than 16 times, and in some such blocks one id occurs exactly 16 times. `latent_ids`: the 32 ids of a row are all different.
All inputs are finite; a program needn't handle non-finite values.
Results may differ from the reference program's by a relative error of at most 0.014.
Values may be sent and summed in bfloat16 or wider, within the bound.
No kernel may reach another device: no remote copies, remote signals or barrier semaphores. Data moves between devices by JAX's collectives and lax.ppermute only.
A program may use at most 192 MiB of HBM per device.

```python
import math
import jax
import jax.numpy as jnp
import numpy as np
from jax import lax

D = 2048
LAT = 8192
K = 32
TOK_DEV = 256
EXPERTS = 32
TOKENS = 8192
CAP = 16


def draw_latent_ids(key, part):
    scores = jax.random.randint(key, (TOKENS, LAT), 0, 131072, dtype=jnp.int32) * LAT + jnp.arange(LAT, dtype=jnp.int32)[None, :]
    top_scores, chosen = lax.top_k(scores, K)
    return chosen.astype(jnp.int32)


def steps_of(stream_key, dims, split, smallest, top_value):
    factor_of = 1.0
    for position, blocks in split:
        steps = jax.random.uniform(jax.random.fold_in(jax.random.fold_in(stream_key, 6), position), (blocks,), jnp.float32, smallest / len(split), top_value / len(split))
        factor_of = factor_of * jnp.repeat(jnp.exp(steps), dims[position] // blocks).reshape((-1,) + (1,) * (len(dims) - 1 - position))
    return factor_of


def deal_out(own_key, own, number, rows, number_of, top, bound, slope):
    sequence = jax.random.permutation(own_key, number_of)
    packed, common = shares(number_of, rows * top, bound, slope, True), shares(number_of, rows * top, bound, slope, False)
    places = jnp.arange(number_of)

    def named(lengths, offset_by):
        used = int((lengths > 0).sum())
        fixed = max(1, used // 4)
        passed = fixed + (places - fixed + offset_by * (used - fixed)) % max(1, number_of - fixed)
        return jnp.zeros((number_of,), jnp.int32).at[sequence[jnp.where(places < fixed, places, passed)]].set(jnp.asarray(lengths, jnp.int32))

    lengths = jnp.where(number % 4 == 0, named(packed, number // 4), named(common, number - number // 4 - 1))
    mixed = jax.random.permutation(jax.random.fold_in(own, 3), number_of)
    giver, sink = mixed[0:number_of // 2 * 2:2], mixed[1:number_of // 2 * 2:2]
    margin = jnp.minimum(lengths[giver] - 1, bound - lengths[sink]) // 2
    margin = jnp.where((giver == sequence[0]) | (sink == sequence[0]) | (lengths[sink] == 0), 0, jnp.maximum(margin, 0))
    passed = jax.random.randint(jax.random.fold_in(own, 4), (number_of // 2,), 0, 1 << 20) % (margin + 1)
    lengths = lengths.at[giver].add(-passed).at[sink].add(passed)
    labels = jnp.searchsorted(jnp.cumsum(lengths), jnp.arange(rows * top), side="right").astype(jnp.int32)
    table = labels.reshape(top, rows).T
    table = table[jax.random.permutation(jax.random.fold_in(own, 1), rows)]
    offset_by = jax.random.randint(jax.random.fold_in(own, 2), (rows, 1), 0, top)
    return jnp.take_along_axis(table, (jnp.arange(top)[None, :] + offset_by) % top, axis=1)


def shares(number_of, total, most, lean, full):
    portions = [(1 << 20) // math.isqrt(grade ** lean) + 1 for grade in range(1, number_of + 1)]
    largest = most if full else min(most, max(-(-total // number_of), total * portions[0] // sum(portions)))
    least = 1 if total - largest >= number_of - 1 else 0
    holding, spare = [largest] + [least] * (number_of - 1), total - largest - least * (number_of - 1)
    while spare > 0:
        free = [i for i in range(1, number_of) if holding[i] < largest] or [i for i in range(1, number_of) if holding[i] < most]
        whole, budget = sum([portions[i] for i in free]), spare
        for i in free:
            extra = min(most - holding[i], max(1, budget * portions[i] // whole), spare)
            holding[i] = holding[i] + extra
            spare = spare - extra
    return np.array(holding)


def normal_values(rng, extent, deviation, limit, shards=(), kind=jnp.bfloat16):
    level = steps_of(rng, extent, shards, -0.22, 0.18) if shards else 1.0
    drawn = jax.random.normal(rng, extent, jnp.float32) * deviation * level
    return jnp.minimum(jnp.maximum(drawn, -limit), limit).astype(kind)


def setup_inputs(seed: int = 0) -> dict:
    key_of = jax.random.split(jax.random.key(seed), 9)
    tokens = normal_values(key_of[0], (TOKENS, D), 1.0, 6.0, ((0, 32),))
    targets = normal_values(key_of[1], (TOKENS, D), 1.0, 6.0, ((0, 32),))
    expert_ids_keys = jax.random.split(jax.random.fold_in(key_of[2], 1), TOKENS // TOK_DEV)
    expert_ids_turns = jax.random.permutation(jax.random.fold_in(key_of[2], 3), TOKENS // TOK_DEV)
    expert_ids = jax.vmap(lambda own, number: deal_out(jax.random.fold_in(key_of[2], 2), own, number, TOK_DEV, EXPERTS, 1, CAP, 2))(expert_ids_keys, expert_ids_turns).reshape((TOKENS, 1))
    latent_ids = draw_latent_ids(jax.random.fold_in(key_of[8], 71), 0)
    w_enc = normal_values(key_of[4], (EXPERTS, D, LAT), D ** -0.5, 0.125, ((0, 32),))
    b_enc = normal_values(key_of[5], (EXPERTS, LAT), 1.0, 4.0, ((0, 32),), jnp.float32)
    w_dec = normal_values(key_of[6], (EXPERTS, LAT, D), K ** -0.5, 1.0, ((0, 32),))
    b_dec = normal_values(key_of[7], (EXPERTS, D), 1.0, 4.0, ((0, 32),), jnp.float32)
    return dict(tokens=tokens, targets=targets, expert_ids=expert_ids, latent_ids=latent_ids, w_enc=w_enc, b_enc=b_enc, w_dec=w_dec, b_dec=b_dec)


def reference(tokens, targets, expert_ids, latent_ids, w_enc, b_enc, w_dec, b_dec):
    row_block = 64
    router = expert_ids[:, 0]

    def one_block(pieces):
        resident_rows, router_here, chosen = pieces
        encoder_weight_columns = w_enc[router_here[:, None], :, chosen]
        preactivation_values = jnp.einsum("rc,rpc->rp", resident_rows.astype(jnp.float32), encoder_weight_columns.astype(jnp.float32))
        latent_activity = jax.nn.relu(preactivation_values + b_enc[router_here[:, None], chosen]).astype(jnp.bfloat16)
        decoder_weight_rows = w_dec[router_here[:, None], chosen]
        gradient_total = jnp.einsum("gc,gcl->gl", latent_activity.astype(jnp.float32), decoder_weight_rows.astype(jnp.float32))
        rebuilt = (gradient_total + b_dec[router_here]).astype(jnp.bfloat16)
        return latent_activity, rebuilt

    latent_activity, rebuilt = lax.map(one_block, (tokens.reshape(-1, row_block, D), router.reshape(-1, row_block), latent_ids.reshape(-1, row_block, K)))
    latent_activity = latent_activity.reshape(TOKENS, K)
    rebuilt = rebuilt.reshape(TOKENS, D)
    residual = (rebuilt.astype(jnp.float32) - targets.astype(jnp.float32)).astype(jnp.bfloat16)
    target_rows = (router[:, None] * LAT + latent_ids).astype(jnp.int32).reshape(-1)
    col_block = math.gcd(D, 256)

    def one_columns(resid_cols):
        products = (latent_activity.astype(jnp.float32)[:, :, None] * resid_cols.astype(jnp.float32)[:, None, :]).reshape(TOKENS * K, col_block)
        return jax.ops.segment_sum(products, target_rows, num_segments=EXPERTS * LAT).astype(jnp.bfloat16)

    col_parts = lax.map(one_columns, jnp.moveaxis(residual.reshape(TOKENS, D // col_block, col_block), 1, 0))
    grad_dec = jnp.moveaxis(col_parts, 0, 1).reshape(EXPERTS, LAT, D)
    return rebuilt, grad_dec
```

```python
import functools

import jax
import jax.numpy as jnp
from jax import lax
from jax.experimental import pallas as pl
from jax.experimental.pallas import tpu as pltpu
from jax.sharding import PartitionSpec as P

F32, BF16, I32 = jnp.float32, jnp.bfloat16, jnp.int32
OVER_ROWS = (((0,), (0,)), ((), ()))


def word_count(latents):
    return max(128, -(-latents // 32))


def id_columns(chosen):
    return -(-2 * chosen // 128) * 128


def slot_table(slot, slots):
    rows = lax.broadcasted_iota(I32, (slots, slot.shape[1]), 0)
    return (rows == slot).astype(F32).astype(BF16)


def pack_kernel(owners, router, ids, tokens, rows_out, slot_out):
    count, columns = tokens.shape
    slots, chosen = rows_out.shape[0], ids.shape[0]
    route = router[...]
    mine = lax.broadcasted_iota(I32, (owners, count), 0) == route
    upper = (
        lax.broadcasted_iota(I32, (count, count), 0) <= lax.broadcasted_iota(I32, (count, count), 1)
    ).astype(F32).astype(BF16)
    running = jnp.dot(mine.astype(F32).astype(BF16), upper, preferred_element_type=F32)
    arrival = jnp.sum(jnp.where(mine, running, 0.0), axis=0, keepdims=True).astype(I32) - 1
    slot = route * (slots // owners) + arrival
    slot_out[...] = slot
    table = slot_table(slot, slots)
    rows_out[:, :columns] = jnp.dot(table, tokens[...], preferred_element_type=F32).astype(BF16)
    marked = ids[...] + 1
    spare = jnp.zeros((rows_out.shape[1] - columns - 2 * chosen, count), BF16)
    pair = jnp.concatenate(
        [(marked >> 7).astype(F32).astype(BF16), (marked & 127).astype(F32).astype(BF16), spare],
        axis=0,
    )
    rows_out[:, columns:] = lax.dot_general(
        table, pair, (((1,), (1,)), ((), ())), preferred_element_type=F32
    ).astype(BF16)


def pack(router, ids, tokens, owners, slots):
    columns = tokens.shape[1] + id_columns(ids.shape[0])
    return pl.pallas_call(
        functools.partial(pack_kernel, owners),
        out_shape=(
            jax.ShapeDtypeStruct((slots, columns), BF16),
            jax.ShapeDtypeStruct(router.shape, I32),
        ),
        name="pack",
    )(router, ids, tokens)


def read_ids(columns, chosen):
    pair = columns.astype(F32)
    return (pair[:, :chosen] * 128.0 + pair[:, chosen : 2 * chosen]).astype(I32) - 1


def coder_kernel(
    words_n, chosen, rows, w_enc, b_enc, w_dec, b_dec, acts_out, recon_out, words, total
):
    step = pl.program_id(0)
    slots, width = acts_out.shape
    columns = w_enc.shape[0]
    per_step = width // words_n

    @pl.when(step == 0)
    def _():
        pair = rows[:, columns:].astype(F32).T
        found = (pair[:chosen] * 128.0 + pair[chosen : 2 * chosen]).astype(I32) - 1
        word_of = jnp.where(found >= 0, found % words_n, -1)
        bit_of = jnp.where(found >= 0, jnp.left_shift(1, jnp.maximum(found, 0) // words_n), 0)
        pieces = []
        for start in range(0, words_n, 64):
            place = lax.broadcasted_iota(I32, (64, slots), 0) + start
            built = jnp.zeros((64, slots), I32)
            for k in range(chosen):
                built = built | jnp.where(word_of[k : k + 1] == place, bit_of[k : k + 1], 0)
            pieces.append(built)
        words[...] = jnp.concatenate(pieces, axis=0).T
        total[...] = jnp.zeros_like(total)

    for part in range(per_step):
        span = slice(part * words_n, (part + 1) * words_n)
        pre = jnp.dot(rows[:, :columns], w_enc[:, span], preferred_element_type=F32)
        bit = jnp.left_shift(1, step * per_step + part)
        acts_out[:, span] = jnp.where(
            (words[...] & bit) != 0, jnp.maximum(pre + b_enc[:, span], 0.0), 0.0
        ).astype(BF16)
    total[...] += jnp.dot(acts_out[...], w_dec[...], preferred_element_type=F32)

    @pl.when(step == pl.num_programs(0) - 1)
    def _():
        recon_out[...] = (total[...] + b_dec[...]).astype(BF16)


def code(chosen, rows, w_enc, b_enc, w_dec, b_dec):
    slots = rows.shape[0]
    columns, latents = w_enc.shape
    words_n = word_count(latents)
    width = min(latents, 4 * words_n)
    whole = lambda shape: pl.BlockSpec(shape, lambda i: (0, 0))
    return pl.pallas_call(
        functools.partial(coder_kernel, words_n, chosen),
        grid=(latents // width,),
        in_specs=[
            whole(rows.shape),
            pl.BlockSpec((columns, width), lambda i: (0, i)),
            pl.BlockSpec((1, width), lambda i: (0, i)),
            pl.BlockSpec((width, columns), lambda i: (i, 0)),
            whole((1, columns)),
        ],
        out_specs=(
            pl.BlockSpec((slots, width), lambda i: (0, i)),
            whole((slots, columns)),
        ),
        out_shape=(
            jax.ShapeDtypeStruct((slots, latents), BF16),
            jax.ShapeDtypeStruct((slots, columns), BF16),
        ),
        scratch_shapes=[pltpu.VMEM((slots, words_n), I32), pltpu.VMEM((slots, columns), F32)],
        cost_estimate=pl.CostEstimate(
            flops=4 * slots * columns * latents,
            bytes_accessed=4 * columns * latents + 2 * slots * latents,
            transcendentals=0,
        ),
        name="coder",
    )(rows, w_enc, b_enc, w_dec, b_dec)


def code_in_parts(chosen, rows, w_enc, b_enc, w_dec, b_dec):
    columns, latents = w_enc.shape
    rows, ids = rows[:, :columns], read_ids(rows[:, columns:], chosen)
    words_n = word_count(latents)
    local = ids - lax.axis_index("latent") * latents
    usable = (ids >= 0) & (local >= 0) & (local < latents)
    word_of = jnp.where(usable, local % words_n, -1)
    bit_of = jnp.where(usable, jnp.left_shift(1, jnp.clip(local, 0, latents - 1) // words_n), 0)
    hits = word_of[:, :, None] == jnp.arange(words_n, dtype=I32)[None, None, :]
    words = jnp.sum(jnp.where(hits, bit_of[:, :, None], 0), axis=1)
    bits = jnp.arange(latents // words_n, dtype=I32)
    mask = (jnp.right_shift(words[:, None, :], bits[None, :, None]) & 1).reshape(-1, latents) != 0
    pre = lax.psum(jnp.dot(rows, w_enc, preferred_element_type=F32), "mp")
    acts = jnp.where(mask, jnp.maximum(pre + b_enc, 0.0), 0.0).astype(BF16)
    total = lax.psum(jnp.dot(acts, w_dec, preferred_element_type=F32), "latent")
    return acts, (total + b_dec).astype(BF16)


def per_device(tokens, targets, expert_ids, latent_ids, w_enc, b_enc, w_dec, b_dec):
    owners = lax.axis_size("expert")
    split = lax.axis_size("latent") * lax.axis_size("mp") > 1
    count, _ = tokens.shape
    cap = 2 * count // owners
    slots = owners * cap

    def exchange(packed):
        blocks = packed.reshape(owners, cap, -1)
        return lax.all_to_all(blocks, "expert", split_axis=0, concat_axis=0, tiled=True).reshape(
            slots, -1
        )

    chosen = latent_ids.shape[1]
    sent_rows, slot = pack(expert_ids.reshape(1, count), latent_ids.T, tokens, owners, slots)
    rows = exchange(sent_rows)
    sent_targets = jnp.dot(
        slot_table(slot, slots), targets, preferred_element_type=F32
    ).astype(BF16)
    wanted = exchange(sent_targets)
    acts, recon = (code_in_parts if split else code)(chosen, rows, w_enc[0], b_enc, w_dec[0], b_dec)
    returned = exchange(recon)
    residual = (recon.astype(F32) - wanted.astype(F32)).astype(BF16)
    grad_dec = lax.dot_general(acts, residual, OVER_ROWS, preferred_element_type=F32)
    rebuilt = lax.dot_general(
        slot_table(slot, slots), returned, OVER_ROWS, preferred_element_type=F32
    )
    return rebuilt.astype(BF16), grad_dec.astype(BF16)[None]


def solution(mesh):
    placed = (
        P("expert", "mp"),
        P("expert", "mp"),
        P("expert", None),
        P("expert", None),
        P("expert", "mp", "latent"),
        P("expert", "latent"),
        P("expert", "latent", "mp"),
        P("expert", "mp"),
    )
    return jax.shard_map(
        per_device,
        mesh=mesh,
        in_specs=placed,
        out_specs=(P("expert", "mp"), P("expert", "latent", "mp")),
        check_vma=False,
    )
```
